32 devices in a mesh: rep: 1, dp: 32 (over x, y, z, core).
Axes of the slice: x: 2, y: 2, z: 4, core: 2. Of those that a mesh axis runs over, the one named last changes fastest.
Arguments:
- x: bfloat16 [32, 2048, 1024], P(('rep', 'dp'))
- dy: bfloat16 [32, 2048, 1024], P(('rep', 'dp'))
- w_gate: bfloat16 [2, 1024, 4096], P(None, 'dp')
- w_up: bfloat16 [2, 1024, 4096], P(None, 'dp')
- w_down: bfloat16 [2, 4096, 1024], P(None, 'dp')
Outputs:
- output 1: bfloat16 [32, 2048, 1024], P(('rep', 'dp'))
- output 2: bfloat16 [2, 1024, 4096], P('rep', 'dp')
- output 3: bfloat16 [2, 1024, 4096], P('rep', 'dp')
- output 4: bfloat16 [2, 4096, 1024], P('rep', 'dp')
All inputs are finite; a program needn't handle non-finite values.
Results may differ from the reference program's by a relative error of at most 0.018.
Values are sent between devices in bfloat16 or wider.
A program may use at most 2 GiB of HBM per device.

```python
import jax
import jax.numpy as jnp
from jax import lax

SEQUENCES = 32
TOKENS = 2048
D = 1024
FF = 4096
LAYERS = 2
NAMES = ("w_gate", "w_up", "w_down")
SHAPES = {"w_gate": (LAYERS, D, FF), "w_up": (LAYERS, D, FF), "w_down": (LAYERS, FF, D)}


def bump(key, n, height):
    away = (jnp.arange(n, dtype=jnp.int32) - jax.random.randint(key, (), 0, n, jnp.int32)) % n
    return jnp.where(away < n // 8, height, 1.0)


def together(key, own, strength):
    shared = jax.random.normal(key, own.shape[1:], jnp.float32)
    return (own + strength * shared) * lax.rsqrt(1 + strength * strength)


def setup_inputs(seed: int = 0, part: int = 0) -> dict:
    kx, kdy, ka, kb, kz, kf, kh, kl, *kw = jax.random.split(jax.random.key(seed), 8 + len(NAMES))
    kx, kdy, ka, kb = (jax.random.fold_in(k, part) for k in (kx, kdy, ka, kb))
    shape = (SEQUENCES, TOKENS, D)
    much_x, much_dy = jax.random.uniform(kz, (2,), jnp.float32, 0.0, 1.0)
    layers = 2.0 ** jax.random.uniform(kl, (LAYERS, 1, 1), jnp.float32, -1.0, 1.0)
    x = together(ka, jax.random.normal(kx, shape, jnp.float32), much_x) * bump(kf, D, 4.0)
    dy = together(kb, jax.random.normal(kdy, shape, jnp.float32), much_dy)
    drawn = {"x": x.astype(jnp.bfloat16), "dy": (dy * (SEQUENCES * TOKENS) ** -0.5).astype(jnp.bfloat16)}
    for key, name in zip(kw, NAMES, strict=True):
        w = jax.random.normal(key, SHAPES[name], jnp.float32) * SHAPES[name][1] ** -0.5
        drawn[name] = (w * {"w_gate": 1.0, "w_up": bump(kh, FF, 4.0), "w_down": layers}[name]).astype(jnp.bfloat16)
    return drawn


def matmul(a, w):
    return jnp.dot(a, w, preferred_element_type=jnp.float32).astype(jnp.bfloat16)


def normed(h):
    wide = h.astype(jnp.float32)
    scale = lax.rsqrt(jnp.mean(wide**2, -1, keepdims=True) + 1e-6)
    return (wide * scale).astype(jnp.bfloat16)


def layer(h, w):
    a = normed(h)
    gate = jnp.dot(a, w["w_gate"], preferred_element_type=jnp.float32)
    up = jnp.dot(a, w["w_up"], preferred_element_type=jnp.float32)
    return h + matmul((jax.nn.silu(gate) * up).astype(jnp.bfloat16), w["w_down"])


def stack(weights, h):
    return lax.scan(lambda h, w: (layer(h, w), None), h, weights)[0]


def reference(x, dy, w_gate, w_up, w_down):
    weights = dict(zip(NAMES, (w_gate, w_up, w_down), strict=True))

    def take(so_far, sequence):
        h, by_y = sequence
        _, back = jax.vjp(stack, weights, h)
        by_weights, by_h = back(by_y)
        return jax.tree.map(lambda total, term: total + term.astype(jnp.float32), so_far, by_weights), by_h

    none_yet = {name: jnp.zeros(w.shape, jnp.float32) for name, w in weights.items()}
    by_weights, by_x = lax.scan(take, none_yet, (x, dy))
    return (by_x, *(by_weights[name].astype(jnp.bfloat16) for name in NAMES))
```

```python
import jax
import jax.numpy as jnp
from jax import lax
from jax.sharding import PartitionSpec as P

BF = jnp.bfloat16
F32 = jnp.float32


def dot(a, b, dims):
    return lax.dot_general(a, b, (dims, ((), ())), preferred_element_type=F32)


NN = ((1,), (0,))
NT = ((1,), (1,))
TN = ((0,), (0,))


def normed(h):
    wide = h.astype(F32)
    scale = lax.rsqrt(jnp.mean(wide**2, -1, keepdims=True) + 1e-6)
    return (wide * scale).astype(BF), scale


def norm_back(h, scale, da):
    wide, da = h.astype(F32), da.astype(F32)
    inner = jnp.mean(da * wide, -1, keepdims=True)
    return scale * da - wide * (scale * scale * scale * inner)


def act_back(gate, up, dhid):
    s = jax.nn.sigmoid(gate)
    silu = gate * s
    return (dhid * up * (s + silu * (1 - s))).astype(BF), (dhid * silu).astype(BF)


def solution(mesh):
    axes = ("rep", "dp")

    def gather(w):
        return lax.all_gather(w, "dp", axis=0, tiled=True)

    def scatter(term):
        return lax.psum_scatter(term, "dp", scatter_dimension=0, tiled=True)

    def step(x, dy, w_gate, w_up, w_down):
        h, dh = x[0], dy[0]
        layers = w_gate.shape[0]
        full = [[gather(w[l]) for w in (w_gate, w_up, w_down)] for l in range(layers)]
        saved = []
        for l in range(layers):
            wg, wu, wd = full[l]
            a, scale = normed(h)
            gate, up = dot(a, wg, NN), dot(a, wu, NN)
            hid = (jax.nn.silu(gate) * up).astype(BF)
            saved.append((h, scale, a, gate, up, hid))
            if l < layers - 1:
                h = h + dot(hid, wd, NN).astype(BF)
        grads = [None] * layers
        for l in reversed(range(layers)):
            wg, wu, wd = full[l]
            h, scale, a, gate, up, hid = saved[l]
            dwd = scatter(dot(hid, dh, TN).astype(BF))
            dhid = dot(dh, wd, NT).astype(BF).astype(F32)
            dgate, dup = act_back(gate, up, dhid)
            dwg = scatter(dot(a, dgate, TN).astype(BF))
            dwu = scatter(dot(a, dup, TN).astype(BF))
            da = dot(dgate, wg, NT).astype(BF) + dot(dup, wu, NT).astype(BF)
            dh = dh + norm_back(h, scale, da).astype(BF)
            grads[l] = (dwg, dwu, dwd)
        return (dh[None], *(jnp.stack(g) for g in zip(*grads)))

    seqs, rows = P(axes, None, None), P(None, "dp", None)
    outs = P("rep", "dp", None)
    return jax.shard_map(
        step, mesh=mesh, in_specs=(seqs, seqs, rows, rows, rows), out_specs=(seqs, outs, outs, outs), check_vma=False
    )
```

```python
import jax
import jax.numpy as jnp
from jax import lax
from jax.sharding import PartitionSpec as P

BF = jnp.bfloat16
F32 = jnp.float32

X, Y, ZH, ZL, CORE = range(5)
OUTWARD = ((CORE, X, Y, ZH, ZL), (CORE, Y, X, ZH, ZL))


def swap(v, bit):
    mask = 16 >> bit
    return lax.ppermute(v, "dp", [(i, i ^ mask) for i in range(32)])


def side(bit):
    return (lax.axis_index("dp") >> (4 - bit)) & 1


def halves_sum(term, order):
    rows, cols = term.shape
    parts = [term.reshape(2, 2, 2, 2, 2, rows // 32, cols)]
    for step, bit in enumerate(order):
        at = side(bit)
        away = [lax.dynamic_index_in_dim(p, 1 - at, bit) for p in parts]
        here = [lax.dynamic_index_in_dim(p, at, bit) for p in parts]
        got = yield sum(p.astype(F32) for p in away).astype(BF), bit, 2 if step == 1 else 1
        parts = [*here, got]
    return sum(p.astype(F32) for p in parts).astype(BF).reshape(rows // 32, cols)


def doubled(block, order):
    rows, cols = block.shape
    held = block.reshape(1, 1, 1, 1, 1, rows, cols)
    for bit in reversed(order):
        got = yield held, bit, 1
        low = side(bit) == 0
        held = jnp.concatenate([jnp.where(low, held, got), jnp.where(low, got, held)], bit)
    return held.reshape(32 * rows, cols)


class Traffic:
    def __init__(self):
        self.active, self.results = {}, {}

    def add(self, name, steps):
        self.active[name] = [steps, None, 0]

    def tick(self, value):
        for chain in self.active.values():
            chain[2] -= 1
        due = [n for n, chain in self.active.items() if chain[2] <= 0]
        got = {n: self.active[n][1] for n in due if self.active[n][1] is not None}
        if got:
            got, value = lax.optimization_barrier((got, value))
        sent = {}
        for n in due:
            try:
                sent[n], *self.active[n][1:] = self.active[n][0].send(got.get(n))
            except StopIteration as end:
                self.results[n] = end.value
                del self.active[n]
        if sent:
            sent, value = lax.optimization_barrier((sent, value))
        for n, v in sent.items():
            bit, ticks = self.active[n][1:]
            self.active[n][1:] = [swap(v, bit), ticks]
        return value

    def finish(self, name, value):
        while name in self.active:
            value = self.tick(value)
        return self.results[name], value


def dot(a, b, dims):
    return lax.dot_general(a, b, (dims, ((), ())), preferred_element_type=F32)


NN = ((1,), (0,))
NT = ((1,), (1,))
TN = ((0,), (0,))


def normed(h):
    wide = h.astype(F32)
    scale = lax.rsqrt(jnp.mean(wide**2, -1, keepdims=True) + 1e-6)
    return (wide * scale).astype(BF), scale


def norm_back(h, scale, da):
    wide, da = h.astype(F32), da.astype(F32)
    inner = jnp.mean(da * wide, -1, keepdims=True)
    return scale * da - wide * (scale * scale * scale * inner)


def act_back(gate, up, dhid):
    s = jax.nn.sigmoid(gate)
    silu = gate * s
    return (dhid * up * (s + silu * (1 - s))).astype(BF), (dhid * silu).astype(BF)


def solution(mesh):
    axes = ("rep", "dp")

    def gather(w):
        return lax.all_gather(w, "dp", axis=0, tiled=True)

    def scatter(term):
        return lax.psum_scatter(term, "dp", scatter_dimension=0, tiled=True)

    def step(x, dy, w_gate, w_up, w_down):
        x, dy = x[0], dy[0]
        line = Traffic()
        wg0, wd0, wu1 = gather(w_gate[0]), gather(w_down[0]), gather(w_up[1])
        line.add("wu0", doubled(w_up[0], OUTWARD[0]))
        line.add("wg1", doubled(w_gate[1], OUTWARD[1]))
        line.add("wd1", doubled(w_down[1], OUTWARD[0]))
        a0, scale0 = normed(x)
        for _ in range(4):
            a0 = line.tick(a0)
        gate0 = dot(a0, wg0, NN)
        wu0, gate0 = line.finish("wu0", gate0)
        up0 = dot(a0, wu0, NN)
        hid0 = (jax.nn.silu(gate0) * up0).astype(BF)
        h1 = x + dot(hid0, wd0, NN).astype(BF)
        a1, scale1 = normed(h1)
        wg1, a1 = line.finish("wg1", a1)
        wd1, a1 = line.finish("wd1", a1)
        gate1 = dot(a1, wg1, NN)
        dhid1 = dot(dy, wd1, NT).astype(BF)
        up1 = dot(a1, wu1, NN)
        hid1 = (jax.nn.silu(gate1) * up1).astype(BF)
        dgate1, dup1 = act_back(gate1, up1, dhid1.astype(F32))

        term, dgate1 = lax.optimization_barrier((dot(hid1, dy, TN).astype(BF), dgate1))
        dwd1 = scatter(term)
        term, dup1 = lax.optimization_barrier((dot(a1, dgate1, TN).astype(BF), dup1))
        dwg1 = scatter(term)
        line.add("dwu1", halves_sum(dot(a1, dup1, TN).astype(BF), OUTWARD[0]))
        dgate1 = line.tick(dgate1)
        da = dot(dgate1, wg1, NT).astype(BF)
        da, dup1 = line.tick((da, dup1))
        da = da + dot(dup1, wu1, NT).astype(BF)
        dh = dy + norm_back(h1, scale1, da).astype(BF)

        dh = line.tick(dh)
        line.add("dwd0", halves_sum(dot(hid0, dh, TN).astype(BF), OUTWARD[1]))
        dh = line.tick(dh)
        dhid0 = dot(dh, wd0, NT).astype(BF).astype(F32)
        dgate0, dup0 = act_back(gate0, up0, dhid0)
        dgate0, dup0 = line.tick((dgate0, dup0))
        line.add("dwg0", halves_sum(dot(a0, dgate0, TN).astype(BF), OUTWARD[0]))
        dgate0, dup0 = line.tick((dgate0, dup0))
        line.add("dwu0", halves_sum(dot(a0, dup0, TN).astype(BF), OUTWARD[1]))
        dgate0, dup0 = line.tick((dgate0, dup0))
        da = dot(dgate0, wg0, NT).astype(BF)
        da, dup0 = line.tick((da, dup0))
        da = da + dot(dup0, wu0, NT).astype(BF)
        dx = dh + norm_back(x, scale0, da).astype(BF)
        for name in ("dwu1", "dwd0", "dwg0", "dwu0"):
            _, dx = line.finish(name, dx)
        done = line.results
        return (
            dx[None],
            jnp.stack([done["dwg0"], dwg1]),
            jnp.stack([done["dwu0"], done["dwu1"]]),
            jnp.stack([done["dwd0"], dwd1]),
        )

    seqs, rows = P(axes, None, None), P(None, "dp", None)
    outs = P("rep", "dp", None)
    return jax.shard_map(
        step, mesh=mesh, in_specs=(seqs, seqs, rows, rows, rows), out_specs=(seqs, outs, outs, outs), check_vma=False
    )
```
